32 devices in a mesh: dp: 2 (over z, core), sp: 16 (over x, y).
Axes of the slice: x: 4, y: 4, z: 1, core: 2. Of those that a mesh axis runs over, the one named last changes fastest.
The devices are a block of a 4x4x8 slice.
Arguments:
- x: bfloat16 [16384, 1152], P(('dp', 'sp')), parts along dimension 0
- gain: bfloat16 [1152], replicated
- wq: bfloat16 [1152, 1024], replicated
- wk: bfloat16 [1152, 256], replicated
- wv: bfloat16 [1152, 256], replicated
- wo: bfloat16 [1024, 1152], replicated
Outputs:
- output: bfloat16 [16384, 1152], P(('dp', 'sp')), parts along dimension 0
There are 2 independent parts. The reference program is written for one: setup_inputs(seed, part) draws one part's arguments, and reference() takes and returns one part's arrays. A program takes and returns all parts, laid end to end along the dimension named above; an argument that names none is the same for every part.
All inputs are finite; a program needn't handle non-finite values.
Results may differ from the reference program's by a relative error of at most 0.012.
Values are sent between devices in bfloat16 or wider.
A program may use at most 768 MiB of HBM per device.

```python
import jax
import jax.numpy as jnp
from jax import lax

ROWS = 8192
D = 1152
HEADS = 4
KV_HEADS = 1
HEAD = 256
THETA = 10000


def setup_inputs(seed: int = 0, part: int = 0) -> dict:
    kx, kn, kq, kk, kv, ko = jax.random.split(jax.random.key(seed), 6)

    def weights(key, rows, columns):
        return jax.random.normal(key, (rows, columns), jnp.float32) * rows**-0.5

    drawn = {
        "x": jax.random.normal(jax.random.fold_in(kx, part), (ROWS, D), jnp.float32),
        "gain": 1 + 0.1 * jax.random.normal(kn, (D,), jnp.float32),
        "wq": 2 * weights(kq, D, HEADS * HEAD),
        "wk": 2 * weights(kk, D, KV_HEADS * HEAD),
        "wv": 4 * weights(kv, D, KV_HEADS * HEAD),
        "wo": weights(ko, HEADS * HEAD, D),
    }
    return {k: v.astype(jnp.bfloat16) for k, v in drawn.items()}


def normed(x, gain):
    wide = x.astype(jnp.float32)
    scale = lax.rsqrt(jnp.mean(wide * wide, -1, keepdims=True) + 1e-6)
    return (wide * scale * gain.astype(jnp.float32)).astype(jnp.bfloat16)


def turned(t, place, theta):
    half = t.shape[-1] // 2
    angle = place.astype(jnp.float32)[:, None] * theta ** (-jnp.arange(half, dtype=jnp.float32) / half)
    cos, sin = jnp.cos(angle)[:, None], jnp.sin(angle)[:, None]
    a, b = t[..., :half].astype(jnp.float32), t[..., half:].astype(jnp.float32)
    return jnp.concatenate([a * cos - b * sin, b * cos + a * sin], -1).astype(jnp.bfloat16)


def matmul(a, w):
    return jnp.dot(a, w, preferred_element_type=jnp.float32).astype(jnp.bfloat16)


def einsum(form, a, b):
    return jnp.einsum(form, a.astype(jnp.float32), b.astype(jnp.float32))


def attention(q, k, v):
    scores = einsum("tgsd,ugd->gstu", q, k) * q.shape[-1] ** -0.5
    token = jnp.arange(q.shape[0])
    scores = jnp.where(token[:, None] >= token, scores, -jnp.inf)
    weights = jax.nn.softmax(scores, -1).astype(jnp.bfloat16)
    return einsum("gstu,ugd->tgsd", weights, v).astype(jnp.bfloat16)


def reference(x, gain, wq, wk, wv, wo):
    a, place = normed(x, gain), jnp.arange(ROWS)
    q = turned(matmul(a, wq).reshape(ROWS, HEADS, HEAD), place, THETA).reshape(ROWS, KV_HEADS, -1, HEAD)
    k = turned(matmul(a, wk).reshape(ROWS, KV_HEADS, HEAD), place, THETA)
    v = matmul(a, wv).reshape(ROWS, KV_HEADS, HEAD)
    seen = attention(q, k, v).reshape(ROWS, HEADS * HEAD)
    return (x.astype(jnp.float32) + jnp.dot(seen, wo, preferred_element_type=jnp.float32)).astype(jnp.bfloat16)
```

```python
import math

import jax
import jax.numpy as jnp
import numpy as np
from jax import lax
from jax.experimental import pallas as pl
from jax.experimental.pallas import tpu as pltpu
from jax.sharding import PartitionSpec as P

HEAD = 256
THETA = 10000
EPS = 1e-6
NEG = -1e30
HIDDEN = 2 * NEG
LOG2E = 1.4426950408889634
LOW = 32

AHEAD = (1, 3, 0, 0, 2, 1, 1, 3, 3, 2, 2, 0, 1, 3, 2)
ASIDE = (0, 0, 1, 3, 0, 1, 3, 1, 3, 1, 3, 2, 2, 2, 2)
AHEAD_DIGITS = sum(d * 4**i for i, d in enumerate(AHEAD))
ASIDE_DIGITS = sum(d * 4**i for i, d in enumerate(ASIDE))


def _dot(a, b, ca, cb):
    return lax.dot_general(a, b, (((ca,), (cb,)), ((), ())), preferred_element_type=jnp.float32)


def _kernel(side, x_hbm, gain_hbm, wq_hbm, wk_hbm, wv_hbm, wo_hbm, far_hbm, near_hbm, y_hbm,
            x_v, gain_v, wq_v, wk_v, wv_v, wo_v, far_v, near_v, a_v, cos_v, sin_v, kv, q_v, top_v, mix_v, gap_v, seen_v, y_v,
            load_sem, out_sem, send_sem, recv_sem):
    own, width = x_v.shape
    half = own // 2
    heads = wq_v.shape[1] // HEAD
    cols = heads * own
    bf16 = jnp.bfloat16
    me = lax.axis_index("sp")
    mx, my = me // side, me % side
    xp = ((mx + 1) % side) * side + my
    xm = ((mx + side - 1) % side) * side + my
    yp = mx * side + (my + 1) % side
    ym = mx * side + (my + side - 1) % side

    def load(i, src, dst):
        copy = pltpu.make_async_copy(src, dst, load_sem.at[i])
        copy.start()
        return copy

    halves = [pl.ds(h * half, half) for h in range(2)]
    in_x0 = load(0, x_hbm.at[halves[0]], x_v.at[halves[0]])
    in_gain = load(1, gain_hbm, gain_v)
    in_wk = load(2, wk_hbm, wk_v)
    in_far = load(3, far_hbm.at[me], far_v)
    in_near = load(4, near_hbm, near_v)
    in_wv = load(5, wv_hbm, wv_v)
    in_x1 = load(6, x_hbm.at[halves[1]], x_v.at[halves[1]])
    in_wq = load(7, wq_hbm, wq_v)
    in_wo = load(8, wo_hbm, wo_v)

    barrier = pltpu.get_barrier_semaphore()
    for other in (xp, xm, yp, ym):
        pl.semaphore_signal(barrier, inc=1, device_id={"sp": other}, device_id_type=pl.DeviceIdType.MESH)

    def remote(src, h, part, to, slot):
        there = kv.at[src, h, part]
        return pltpu.make_async_remote_copy(src_ref=there, dst_ref=there, send_sem=send_sem.at[slot], recv_sem=recv_sem.at[src, h, part],
                                            device_id={"sp": to}, device_id_type=pl.DeviceIdType.MESH)

    def slot(h, direction, p, what):
        return ((h * 4 + direction) * 4 + p) * 3 + what

    in_far.wait()
    in_near.wait()
    rot = HEAD // 2
    near_c, near_s = near_v[:, :rot], near_v[:, rot:]
    for i in range(own // LOW):
        far_c, far_s = far_v[i : i + 1, :rot], far_v[i : i + 1, rot:]
        cos_v[i * LOW : (i + 1) * LOW, :] = near_c * far_c - near_s * far_s
        sin_v[i * LOW : (i + 1) * LOW, :] = near_s * far_c + near_c * far_s

    def turned(t, rows):
        t = t.astype(bf16).astype(jnp.float32)
        a, b = t[:, :rot], t[:, rot:]
        cos, sin = cos_v[rows, :], sin_v[rows, :]
        return jnp.concatenate([a * cos - b * sin, b * cos + a * sin], axis=1).astype(bf16)

    in_gain.wait()
    gain = gain_v[...].astype(jnp.float32).reshape(1, width)

    def norm(h):
        wide = x_v[halves[h], :].astype(jnp.float32)
        scale = lax.rsqrt(jnp.mean(wide * wide, -1, keepdims=True) + EPS)
        a_v[halves[h], :] = (wide * scale * gain).astype(bf16)

    def keys(h):
        kv[me, h, 0] = turned(_dot(a_v[halves[h], :], wk_v[...], 1, 0), halves[h])

    def values(h):
        kv[me, h, 1] = _dot(a_v[halves[h], :], wv_v[...], 1, 0).T.astype(bf16)

    def send_own(h, part):
        first, second = ((xp, xm), (yp, ym)) if h == 0 else ((yp, ym), (xp, xm))
        for d in range(2):
            remote(me, h, part, first[d], slot(h, d, 0, part)).start()
            remote(me, h, part, second[d], slot(h, 2 + d, 0, part)).start()

    in_x0.wait()
    norm(0)
    in_wk.wait()
    keys(0)
    in_wv.wait()
    values(0)
    pl.semaphore_wait(barrier, 4)
    send_own(0, 0)
    in_x1.wait()
    norm(1)
    send_own(0, 1)
    keys(1)
    values(1)
    send_own(1, 0)

    in_wq.wait()
    for n in range(heads):
        q = _dot(a_v[...], wq_v[:, n * HEAD : (n + 1) * HEAD], 1, 0)
        q_v[n * own : (n + 1) * own, :] = turned(q, pl.ds(0, own))
        if n == 0:
            send_own(1, 1)

    gap_v[...] = lax.broadcasted_iota(jnp.int32, gap_v.shape, 1) - lax.broadcasted_iota(jnp.int32, gap_v.shape, 0)
    top_v[...] = jnp.full(top_v.shape, NEG, jnp.float32)
    mix_v[...] = jnp.zeros(mix_v.shape, jnp.float32)
    e = HEAD**-0.5 * LOG2E
    ones = jnp.ones((8, half), bf16)

    def attend(src, h, level):
        k, v = kv[src, h, 0], jnp.concatenate([kv[src, h, 1], ones], axis=0)
        strips = [pl.ds(n * own, own) for n in range(heads)]
        scores = [_dot(k, q_v[strip, :], 1, 1) for strip in strips]
        weights, keeps = [], []
        for strip, s in zip(strips, scores):
            if level is not None:
                s = jnp.where(gap_v[...] >= level, s, HIDDEN)
            old = top_v[:, strip]
            top = jnp.maximum(old, s.max(axis=0, keepdims=True))
            top_v[:, strip] = top
            weights.append(jnp.exp2((s - top) * e).astype(bf16))
            keeps.append(jnp.exp2((old - top) * e))
        for strip, p, keep in zip(strips, weights, keeps):
            mix_v[:, strip] = mix_v[:, strip] * keep + _dot(v, p, 1, 0)

    def own_half(h, _):
        attend(me, h, h * half)

    lax.fori_loop(0, 2, own_half, None)

    def step(n, _):
        h, i = n % 2, n // 2
        p, m = (AHEAD_DIGITS >> (2 * i)) % 4, (ASIDE_DIGITS >> (2 * i)) % 4
        dx, dy = p * (1 - h) + m * h, m * (1 - h) + p * h
        src = ((mx + side - dx) % side) * side + (my + side - dy) % side
        first_p, first_m = xp * (1 - h) + yp * h, xm * (1 - h) + ym * h
        second_p, second_m = yp * (1 - h) + xp * h, ym * (1 - h) + xm * h
        for part in range(2):
            remote(src, h, part, xp, 0).wait_recv()

        @pl.when(m == 0)
        def _():
            @pl.when(p == 1)
            def _():
                remote(src, h, 0, first_p, slot(h, 0, 0, 2)).start()

            @pl.when(p == 3)
            def _():
                remote(src, h, 1, first_m, slot(h, 1, 0, 2)).start()

            for part in range(2):
                remote(src, h, part, second_p, slot(h, 2, p, part)).start()
                remote(src, h, part, second_m, slot(h, 3, p, part)).start()

        @pl.when(m == 1)
        def _():
            remote(src, h, 0, second_p, slot(h, 2, p, 2)).start()

        @pl.when(m == 3)
        def _():
            remote(src, h, 1, second_m, slot(h, 3, p, 2)).start()

        @pl.when(src < me)
        def _():
            attend(src, h, None)

    lax.fori_loop(0, 30, step, None)

    in_wo.wait()
    for n in range(heads):
        strip = pl.ds(n * own, own)
        seen_v[:, n * HEAD : (n + 1) * HEAD] = (mix_v[:HEAD, strip] * (1 / mix_v[HEAD : HEAD + 1, strip])).T.astype(bf16)
    outs = []
    for h in range(2):
        y = _dot(seen_v[halves[h], :], wo_v[...], 1, 0)
        y_v[halves[h], :] = (x_v[halves[h], :].astype(jnp.float32) + y).astype(bf16)
        outs.append(pltpu.make_async_copy(y_v.at[halves[h]], y_hbm.at[halves[h]], out_sem.at[h]))
        outs[-1].start()

    def sent(n, _):
        h, direction = n // 8, (n // 2) % 4
        @pl.when(direction < 2)
        def _():
            @pl.when(n % 2 == 0)
            def _():
                for what in range(3):
                    remote(me, 0, 0, xp, slot(h, direction, 0, what)).wait_send()

        @pl.when(direction >= 2)
        def _():
            for j in range(2):
                for what in range(3):
                    remote(me, 0, 0, xp, slot(h, direction, (n % 2) * 2 + j, what)).wait_send()

    lax.fori_loop(0, 16, sent, None)
    for copy in outs:
        copy.wait()


def _tables(places, own):
    turn = THETA ** (-np.arange(HEAD // 2) / (HEAD // 2))
    both = lambda place: np.concatenate([np.cos(place[..., None] * turn), np.sin(place[..., None] * turn)], -1).astype(np.float32)
    return both(np.arange(places * own // LOW).reshape(places, -1) * float(LOW)), both(np.arange(LOW) * 1.0)


def solution(mesh):
    places = mesh.shape["sp"]
    side = math.isqrt(places)
    assert side == 4 and side * side == places

    def step(x, gain, wq, wk, wv, wo):
        own, width = x.shape
        half, cols = own // 2, wq.shape[1] // HEAD * own
        far, near = _tables(places, own)
        bf16, f32 = jnp.bfloat16, jnp.float32
        like = lambda t: pltpu.VMEM(t.shape, t.dtype)
        return pl.pallas_call(
            lambda *refs: _kernel(side, *refs),
            in_specs=[pl.BlockSpec(memory_space=pl.ANY)] * 8,
            out_specs=pl.BlockSpec(memory_space=pl.ANY),
            out_shape=jax.ShapeDtypeStruct(x.shape, bf16),
            scratch_shapes=[
                like(x), like(gain), like(wq), like(wk), like(wv), like(wo),
                pltpu.VMEM(far.shape[1:], f32), pltpu.VMEM(near.shape, f32),
                like(x), pltpu.VMEM((own, HEAD // 2), f32), pltpu.VMEM((own, HEAD // 2), f32),
                pltpu.VMEM((places, 2, 2, half, HEAD), bf16),
                pltpu.VMEM((cols, HEAD), bf16),
                pltpu.VMEM((1, cols), f32), pltpu.VMEM((HEAD + 8, cols), f32), pltpu.VMEM((half, own), jnp.int32),
                pltpu.VMEM((own, wo.shape[0]), bf16), like(x),
                pltpu.SemaphoreType.DMA((9,)), pltpu.SemaphoreType.DMA((2,)),
                pltpu.SemaphoreType.DMA((96,)), pltpu.SemaphoreType.DMA((places, 2, 2)),
            ],
            compiler_params=pltpu.CompilerParams(collective_id=0, has_side_effects=True, vmem_limit_bytes=60 * 2**20),
        )(x, gain, wq, wk, wv, wo, jnp.asarray(far), jnp.asarray(near))

    tokens, whole = P(("dp", "sp"), None), P(None, None)
    return jax.shard_map(step, mesh=mesh, in_specs=(tokens, P(None), whole, whole, whole, whole), out_specs=tokens, check_vma=False)
```
